32 devices in a mesh: dp: 4 (over x, core), mp: 8 (over z, y).
Axes of the slice: x: 2, y: 2, z: 4, core: 2. Of those that a mesh axis runs over, the one named last changes fastest.
Arguments:
- cotangent: bfloat16 [512, 4608], P(('dp', 'mp')), may hold values from -50 to 50
- mlp_out: bfloat16 [512, 4608], P(('dp', 'mp')), may hold values from -500 to 500
- post_gain: float32 [4608], replicated, may hold values from 0.5 to 1.5
- down_weight: bfloat16 [36864, 4608], P('mp', 'dp'), may hold values from -0.09375 to 0.09375
- gate_pre: bfloat16 [512, 36864], P('dp', 'mp'), may hold values from -6 to 6
- up_pre: bfloat16 [512, 36864], P('dp', 'mp'), may hold values from -6 to 6
Outputs:
- gate_grad: float32 [512, 36864], P('dp', 'mp')
- up_grad: float32 [512, 36864], P('dp', 'mp')
- gain_grad: float32 [4608], replicated
The draws below stay inside these ranges and needn't reach their ends.
All inputs are finite; a program needn't handle non-finite values.
Results may differ from the reference program's by a relative error of at most 0.0005.
Values may be sent and summed in bfloat16 or wider, within the bound.
A program may use at most 64 MiB of HBM per device.

```python
import jax
import jax.numpy as jnp
from jax import lax

D = 4608
FF = 36864
TOKENS = 512


def draw_cotangent(key, part):
    noise_key, jitter_key = jax.random.split(jax.random.fold_in(key, 17))
    row_pos = jnp.arange(TOKENS, dtype=jnp.float32)[:, None] / TOKENS
    jitter = jax.random.uniform(jitter_key, (TOKENS, 1), jnp.float32)
    values = jnp.clip(jax.random.normal(noise_key, (TOKENS, D), jnp.float32), -5.0, 5.0)
    row_exp = 0.5 * row_pos + 0.5 * jitter
    return (values * 10.0 ** row_exp).astype(jnp.bfloat16)


def draw_mlp_out(key, part):
    noise_key, row_key, col_key = jax.random.split(jax.random.fold_in(key, 29), 3)
    row_exp = jax.random.uniform(row_key, (TOKENS, 1), jnp.float32)
    col_exp = jax.random.uniform(col_key, (1, D), jnp.float32)
    values = jnp.clip(jax.random.normal(noise_key, (TOKENS, D), jnp.float32), -5.0, 5.0)
    return (values * 10.0 ** row_exp * 10.0 ** col_exp).astype(jnp.bfloat16)


def steps_of(own_key, shape, cuts, smallest, top_value):
    loudness = 1.0
    for dim, parts in cuts:
        heights = jax.random.uniform(jax.random.fold_in(jax.random.fold_in(own_key, 6), dim), (parts,), jnp.float32, smallest / len(cuts), top_value / len(cuts))
        loudness = loudness * jnp.repeat(jnp.exp(heights), shape[dim] // parts).reshape((-1,) + (1,) * (len(shape) - 1 - dim))
    return loudness


def bell_draw(rng, shape, deviation, most, cuts=(), kind=jnp.bfloat16):
    values = jax.random.normal(rng, shape, jnp.float32) * deviation
    if len(cuts) > 0:
        values = steps_of(rng, shape, cuts, -0.22, 0.18) * values
    return jnp.clip(values, min=-most, max=most).astype(kind)


def setup_inputs(seed: int = 0) -> dict:
    arg_keys = jax.random.split(jax.random.key(seed), 7)
    cotangent = draw_cotangent(jax.random.fold_in(arg_keys[6], 71), 0)
    mlp_out = draw_mlp_out(jax.random.fold_in(arg_keys[6], 71), 0)
    post_gain = jnp.clip(1.0 + 0.1 * jax.random.normal(arg_keys[2], (D,), jnp.float32), 0.5, 1.5)
    down_weight = bell_draw(arg_keys[3], (FF, D), D ** -0.5, 0.09375, ((0, 8), (1, 4)))
    gate_pre = bell_draw(arg_keys[4], (TOKENS, FF), 1.0, 6.0, ((0, 4), (1, 8)))
    up_pre = bell_draw(arg_keys[5], (TOKENS, FF), 1.0, 6.0, ((0, 4), (1, 8)))
    return {"cotangent": cotangent, "mlp_out": mlp_out, "post_gain": post_gain, "down_weight": down_weight, "gate_pre": gate_pre, "up_pre": up_pre}


epsilon = 1e-06

def gelu_tanh(values):
    return jax.nn.gelu(values, approximate=True)

def reference(cotangent, mlp_out, post_gain, down_weight, gate_pre, up_pre):
    forward = mlp_out.astype(jnp.float32)
    upstream = cotangent.astype(jnp.float32)
    root_mean = jnp.sqrt(lax.optimization_barrier(jnp.mean(forward * forward, axis=1, keepdims=True)) + epsilon)
    normed = forward / root_mean
    gain_grad = lax.optimization_barrier(jnp.sum(upstream * normed, axis=0))
    scaled = upstream * post_gain[None, :]
    project_sum = lax.optimization_barrier(jnp.sum(scaled * forward, axis=1, keepdims=True))
    out_grad = scaled / root_mean - forward * project_sum / (D * root_mean ** 3)
    hidden_grad = jnp.dot(out_grad, down_weight.astype(jnp.float32).T, precision=lax.Precision.HIGHEST)
    gate_val = gate_pre.astype(jnp.float32)
    up_val = up_pre.astype(jnp.float32)
    act_val, pull_back = jax.vjp(gelu_tanh, gate_val)
    gate_grad = pull_back(hidden_grad * up_val)[0]
    up_grad = hidden_grad * act_val
    return (gate_grad, up_grad, gain_grad)
```

```python
import functools
import math

import jax
import jax.numpy as jnp
from jax import lax
from jax.experimental import pallas as pl
from jax.experimental.pallas import tpu as pltpu
from jax.sharding import PartitionSpec as P

MESH = pl.DeviceIdType.MESH
LANES = 128
WEIGHT_MAX = 0.09375

epsilon = 1e-06


def gelu_tanh(values):
    return jax.nn.gelu(values, approximate=True)


def encode(values, gain):
    v = values * gain
    v2 = v * v
    v4 = v2 * v2
    v8 = v4 * v4
    return jnp.where(v < 0, -v8, v8).astype(jnp.bfloat16)


def decode(codes, gain):
    b = codes.astype(jnp.float32)
    size = jnp.abs(b)
    root = jnp.exp(jnp.log(size) * 0.125) * (1.0 / gain)
    root = jnp.where(size > 0, root, 0.0)
    return jnp.where(b < 0, -root, root)


def kernel(
    dp, mp, gain, tile,
    c_ref, y_ref, post_ref, w_hbm, out_hbm, gain_out,
    w_ref, grad, code, lhs, part, other, sent, got, held, gsum, gsend_a, grecv_a, grecv_b, gblock,
    w_sem, a_send, a_recv, ga_send, ga_recv, g_recv, z_send, y_send, gb_send, gb_recv,
    d_send, d_recv, x_send, x_recv, go_send, go_recv, o_sem,
):
    d, m = lax.axis_index("dp"), lax.axis_index("mp")
    nx, nz = dp // 2, mp // 2
    x, core = d // 2, lax.rem(d, 2)
    z, y = m // 2, lax.rem(m, 2)
    rows, full = c_ref.shape
    feat = full // dp
    hid = w_ref.shape[0]

    def remote(src, dst, send, recv, dev):
        return pltpu.make_async_remote_copy(
            src_ref=src, dst_ref=dst, send_sem=send, recv_sem=recv, device_id=dev, device_id_type=MESH
        )

    w_copy = pltpu.make_async_copy(w_hbm, w_ref, w_sem)
    w_copy.start()

    barrier = pltpu.get_barrier_semaphore()
    for j in range(1, dp):
        pl.semaphore_signal(barrier, inc=1, device_id=(lax.rem(d + j, dp), m), device_id_type=MESH)
    for j in range(1, mp):
        pl.semaphore_signal(barrier, inc=1, device_id=(d, lax.rem(m + j, mp)), device_id_type=MESH)

    forward = y_ref[...].astype(jnp.float32)
    upstream = c_ref[...].astype(jnp.float32)
    inv = 1.0 / jnp.sqrt(jnp.mean(forward * forward, axis=1, keepdims=True) + epsilon)
    normed = forward * inv
    gain_part = jnp.sum(upstream * normed, axis=0, keepdims=True)
    scaled = upstream * post_ref[...]
    mean_prod = jnp.sum(scaled * normed, axis=1, keepdims=True) * (1.0 / full)
    out_grad = (scaled - normed * mean_prod) * inv
    top = jnp.max(jnp.abs(out_grad), axis=1, keepdims=True).astype(jnp.bfloat16).astype(jnp.float32)
    top = jnp.where(top > 1e-37, top, 1.0)
    codes = encode(out_grad * (1.0 / top), gain)
    top_wide = jnp.broadcast_to(top, (rows, LANES)).astype(jnp.bfloat16)
    for t in range(dp):
        code[t, :, :feat] = codes[:, t * feat:(t + 1) * feat]
        code[t, :, feat:] = top_wide
        gsend_a[t] = gain_part[:, t * feat:(t + 1) * feat]
    grad[m, d] = code[d]

    pl.semaphore_wait(barrier, dp - 1 + mp - 1)

    def a_copy(j):
        t = lax.rem(d + j, dp)
        return remote(code.at[t], grad.at[m, d], a_send.at[j], a_recv.at[j], (t, m))

    def ga_copy(j):
        t = lax.rem(d + j, dp)
        return remote(gsend_a.at[t], grecv_a.at[j], ga_send.at[j], ga_recv.at[j], (t, m))

    for j in range(1, dp):
        a_copy(j).start()
    for j in range(1, dp):
        ga_copy(j).start()
    for j in range(1, dp):
        a_copy(j).wait_recv()

    def chunk_z(p):
        odd = lax.rem(p, 2)
        off = odd * ((p + 1) // 2) - (1 - odd) * (p // 2)
        return lax.rem(z + off + nz, nz)

    def chunk(k):
        q = lax.rem(k, 2)
        return 2 * chunk_z(k // 2) + lax.rem(y + q, 2)

    def z_copy(p):
        return remote(grad.at[m], grad.at[m], z_send.at[p], g_recv.at[m], (d, 2 * chunk_z(p) + y))

    def y_copy(p):
        mine = 2 * chunk_z(p) + y
        return remote(grad.at[mine], grad.at[mine], y_send.at[p], g_recv.at[mine], (d, 2 * z + 1 - y))

    def g_wait(mc):
        remote(grad.at[mc], grad.at[mc], y_send.at[0], g_recv.at[mc], (d, 2 * z + 1 - y)).wait_recv()

    y_copy(0).start()
    for p in range(1, nz):
        z_copy(p).start()

    for j in range(1, dp):
        ga_copy(j).wait_recv()
    total = gsend_a[d]
    for j in range(1, dp):
        total = total + grecv_a[j]
    gsum[...] = total

    def gb_copy(j):
        return remote(gsum, grecv_b.at[j], gb_send.at[j], gb_recv.at[j], (d, lax.rem(m + j, mp)))

    for j in range(1, mp):
        gb_copy(j).start()

    w_copy.wait()

    def d_copy(k, xo):
        return remote(
            part.at[k, 2 * xo + 1 - core], other.at[k, xo], d_send.at[k, xo], d_recv.at[k, xo], (2 * x + 1 - core, m)
        )

    def x_copy(k, j):
        return remote(
            sent.at[k, j - 1], got.at[k, j - 1], x_send.at[k, j - 1], x_recv.at[k, j - 1],
            (2 * lax.rem(x + j, nx) + core, m),
        )

    def compute(k):
        mc = chunk(k)
        for t in range(dp):
            value = decode(grad[mc, t][:, :feat], gain)
            high = value.astype(jnp.bfloat16)
            lhs[pl.ds(t * rows, rows), :] = high
            lhs[pl.ds((dp + t) * rows, rows), :] = (value - high.astype(jnp.float32)).astype(jnp.bfloat16)

        def one(i, carry):
            cols = pl.ds(pl.multiple_of(i * tile, tile), tile)
            both = lax.dot_general(
                lhs[...], w_ref[cols, :], (((1,), (1,)), ((), ())), preferred_element_type=jnp.float32
            )
            both = both[: dp * rows] + both[dp * rows:]
            for t in range(dp):
                part[k, t, :, cols] = both[t * rows:(t + 1) * rows]
            return carry

        lax.fori_loop(0, hid // tile, one, 0)
        for j in range(1, nx + 1):
            d_copy(k, lax.rem(x + j, nx)).start()

    def reduce(k):
        for j in range(1, nx):
            xo = lax.rem(x + j, nx)
            d_copy(k, xo).wait_recv()

            def one(i, carry):
                cols = pl.ds(pl.multiple_of(i * tile, tile), tile)
                sent[k, j - 1, :, cols] = encode(part[k, 2 * xo + core, :, cols] + other[k, xo, :, cols], gain)
                return carry

            lax.fori_loop(0, hid // tile, one, 0)
            x_copy(k, j).start()

    def step(k, carry):
        q = lax.rem(k, 2)

        @pl.when(q == 1)
        def _():
            g_wait(chunk(k))

        compute(k)

        @pl.when(jnp.logical_and(q == 0, k + 2 < mp))
        def _():
            g_wait(chunk(k + 2))
            y_copy(k // 2 + 1).start()

        @pl.when(k > 0)
        def _():
            reduce(k - 1)

        return carry

    lax.fori_loop(0, mp, step, 0)
    reduce(mp - 1)

    gtotal = gsum[...]
    for j in range(1, mp):
        gb_copy(j).wait_recv()
        gtotal = gtotal + grecv_b[j]
    gblock[...] = gtotal
    gain_out[d] = gtotal

    def go_copy(j):
        return remote(gblock, gain_out.at[d], go_send.at[j], go_recv.at[j], (lax.rem(d + j, dp), m))

    for j in range(1, dp):
        go_copy(j).start()

    def o_copy(k):
        return pltpu.make_async_copy(held.at[k], out_hbm.at[chunk(k)], o_sem.at[k])

    def finish(k, carry):
        mc = chunk(k)
        d_copy(k, x).wait_recv()
        for j in range(1, nx):
            x_copy(k, j).wait_recv()
        size = grad[mc, d][:, feat:].astype(jnp.float32)[:, :1]

        def one(i, inner):
            cols = pl.ds(pl.multiple_of(i * tile, tile), tile)
            value = part[k, d, :, cols] + other[k, x, :, cols]
            for j in range(1, nx):
                value = value + decode(got[k, j - 1, :, cols], gain)
            held[k, :, cols] = value * size
            return inner

        lax.fori_loop(0, hid // tile, one, 0)
        o_copy(k).start()
        return carry

    lax.fori_loop(0, mp, finish, 0)

    for j in range(1, dp):
        go_copy(j).wait()
        a_copy(j).wait_send()
        ga_copy(j).wait_send()
    for j in range(1, mp):
        gb_copy(j).wait_send()
    for p in range(nz):
        y_copy(p).wait_send()
    for p in range(1, nz):
        z_copy(p).wait_send()

    def drain(k, carry):
        for xo in range(nx):
            d_copy(k, xo).wait_send()
        for j in range(1, nx):
            x_copy(k, j).wait_send()
        o_copy(k).wait()
        return carry

    lax.fori_loop(0, mp, drain, 0)


def fused(dp, mp, cotangent, mlp_out, post_gain, down_weight):
    rows, full = cotangent.shape
    hid, feat = down_weight.shape
    nx, nz = dp // 2, mp // 2
    gain = 2.0 ** math.floor(15.8 - math.log2(full * WEIGHT_MAX))
    tile = next(t for t in (512, 256, 128) if hid % t == 0)
    bf, f32 = jnp.bfloat16, jnp.float32
    dma = pltpu.SemaphoreType.DMA
    hidden, gain_grad = pl.pallas_call(
        functools.partial(kernel, dp, mp, gain, tile),
        out_shape=(jax.ShapeDtypeStruct((mp, rows, hid), f32), jax.ShapeDtypeStruct((dp, 1, feat), f32)),
        in_specs=[pl.BlockSpec(memory_space=pltpu.VMEM)] * 3 + [pl.BlockSpec(memory_space=pl.ANY)],
        out_specs=(pl.BlockSpec(memory_space=pl.ANY), pl.BlockSpec(memory_space=pltpu.VMEM)),
        scratch_shapes=[
            pltpu.VMEM((hid, feat), bf),
            pltpu.VMEM((mp, dp, rows, feat + LANES), bf),
            pltpu.VMEM((dp, rows, feat + LANES), bf),
            pltpu.VMEM((2 * dp * rows, feat), bf),
            pltpu.VMEM((mp, dp, rows, hid), f32),
            pltpu.VMEM((mp, nx, rows, hid), f32),
            pltpu.VMEM((mp, nx - 1, rows, hid), bf),
            pltpu.VMEM((mp, nx - 1, rows, hid), bf),
            pltpu.VMEM((mp, rows, hid), f32),
            pltpu.VMEM((1, feat), f32),
            pltpu.VMEM((dp, 1, feat), f32),
            pltpu.VMEM((dp, 1, feat), f32),
            pltpu.VMEM((mp, 1, feat), f32),
            pltpu.VMEM((1, feat), f32),
            dma, dma((dp,)), dma((dp,)), dma((dp,)), dma((dp,)),
            dma((mp,)), dma((nz,)), dma((nz,)), dma((mp,)), dma((mp,)),
            dma((mp, nx)), dma((mp, nx)), dma((mp, nx)), dma((mp, nx)),
            dma((dp,)), dma((dp,)), dma((mp,)),
        ],
        compiler_params=pltpu.CompilerParams(
            collective_id=0, has_side_effects=True, vmem_limit_bytes=48 * 1024 * 1024
        ),
        name="norm_gather_project_reduce",
    )(cotangent, mlp_out, post_gain.reshape(1, full), down_weight)
    return hidden.reshape(mp * rows, hid), gain_grad.reshape(full)


def plain(cotangent, mlp_out, post_gain, down_weight):
    full = cotangent.shape[1]
    forward = mlp_out.astype(jnp.float32)
    upstream = cotangent.astype(jnp.float32)
    root_mean = jnp.sqrt(jnp.mean(forward * forward, axis=1, keepdims=True) + epsilon)
    normed = forward / root_mean
    gain_part = jnp.sum(upstream * normed, axis=0)
    scaled = upstream * post_gain[None, :]
    project_sum = jnp.sum(scaled * forward, axis=1, keepdims=True)
    out_grad = scaled / root_mean - forward * project_sum / (full * root_mean**3)
    hid_units = down_weight.shape[0]
    gain_grad = lax.psum(gain_part, ("dp", "mp"))
    pieces = lax.all_to_all(out_grad, "dp", split_axis=1, concat_axis=0, tiled=True)
    partial_value = jnp.dot(
        lax.all_gather(pieces, "mp", axis=0, tiled=True),
        down_weight.astype(jnp.float32).T,
        precision=lax.Precision.HIGHEST,
    )
    dp_count = lax.axis_size("dp")
    mp_count = lax.axis_size("mp")
    row_count = out_grad.shape[0]
    partial_value = partial_value.reshape(mp_count, dp_count * row_count, hid_units)
    summed = lax.psum_scatter(partial_value, "dp", scatter_dimension=1, tiled=True)
    return summed.reshape(mp_count * row_count, hid_units), gain_grad


def local(dp, mp, cotangent, mlp_out, post_gain, down_weight, gate_pre, up_pre):
    rows = cotangent.shape[0]
    hid, feat = down_weight.shape
    held_bytes = mp * rows * hid * (4 * dp + 4 * dp // 2 + 2 * dp + 4) + 2 * hid * feat
    tiled = rows % 16 == 0 and hid % LANES == 0 and feat % LANES == 0
    paired = dp % 2 == 0 and mp % 2 == 0 and dp > 2
    if tiled and paired and held_bytes < 40 * 1024 * 1024:
        hidden_grad, gain_grad = fused(dp, mp, cotangent, mlp_out, post_gain, down_weight)
    else:
        hidden_grad, gain_grad = plain(cotangent, mlp_out, post_gain, down_weight)
    gate_val = gate_pre.astype(jnp.float32)
    up_val = up_pre.astype(jnp.float32)
    act_val, pull_back = jax.vjp(gelu_tanh, gate_val)
    gate_grad = pull_back(hidden_grad * up_val)[0]
    up_grad = hidden_grad * act_val
    return (gate_grad, up_grad, gain_grad)


def solution(mesh):
    return jax.shard_map(
        functools.partial(local, mesh.shape["dp"], mesh.shape["mp"]),
        mesh=mesh,
        in_specs=(
            P(("dp", "mp"), None),
            P(("dp", "mp"), None),
            P(),
            P("mp", "dp"),
            P("dp", "mp"),
            P("dp", "mp"),
        ),
        out_specs=(P("dp", "mp"), P("dp", "mp"), P()),
        check_vma=False,
    )
```

```python
import functools
import math

import jax
import jax.numpy as jnp
from jax import lax
from jax.experimental import pallas as pl
from jax.experimental.pallas import tpu as pltpu
from jax.sharding import PartitionSpec as P

MESH = pl.DeviceIdType.MESH
LANES = 128
WEIGHT_MAX = 0.09375

epsilon = 1e-06


def gelu_tanh(values):
    return jax.nn.gelu(values, approximate=True)


def encode(values, gain):
    v = values * gain
    v2 = v * v
    v4 = v2 * v2
    v8 = v4 * v4
    return jnp.where(v < 0, -v8, v8).astype(jnp.bfloat16)


def decode(codes, gain):
    b = codes.astype(jnp.float32)
    size = jnp.abs(b)
    root = jnp.exp(jnp.log(size) * 0.125) * (1.0 / gain)
    root = jnp.where(size > 0, root, 0.0)
    return jnp.where(b < 0, -root, root)


def kernel(
    dp, mp, gain, tile,
    c_ref, y_ref, post_ref, w_hbm, out_ref, gain_out,
    w_ref, grad, code, lhs, part, other, sent, got, gsum, gsend_a, grecv_a, grecv_b, gblock,
    w_sem, a_send, a_recv, ga_send, ga_recv, g_recv, z_send, y_send, gb_send, gb_recv,
    d_send, d_recv, x_send, x_recv, go_send, go_recv,
):
    d, m = lax.axis_index("dp"), lax.axis_index("mp")
    nx, nz = dp // 2, mp // 2
    x, core = d // 2, lax.rem(d, 2)
    z, y = m // 2, lax.rem(m, 2)
    rows, full = c_ref.shape
    feat = full // dp
    half = w_ref.shape[0] // 2

    def remote(src, dst, send, recv, dev):
        return pltpu.make_async_remote_copy(
            src_ref=src, dst_ref=dst, send_sem=send, recv_sem=recv, device_id=dev, device_id_type=MESH
        )

    w_copy = pltpu.make_async_copy(w_hbm, w_ref, w_sem)
    w_copy.start()

    barrier = pltpu.get_barrier_semaphore()
    for j in range(1, dp):
        pl.semaphore_signal(barrier, inc=1, device_id=(lax.rem(d + j, dp), m), device_id_type=MESH)
    for j in range(1, mp):
        pl.semaphore_signal(barrier, inc=1, device_id=(d, lax.rem(m + j, mp)), device_id_type=MESH)

    forward = y_ref[...].astype(jnp.float32)
    upstream = c_ref[...].astype(jnp.float32)
    inv = 1.0 / jnp.sqrt(jnp.mean(forward * forward, axis=1, keepdims=True) + epsilon)
    normed = forward * inv
    gain_part = jnp.sum(upstream * normed, axis=0, keepdims=True)
    scaled = upstream * post_ref[...]
    mean_prod = jnp.sum(scaled * normed, axis=1, keepdims=True) * (1.0 / full)
    out_grad = (scaled - normed * mean_prod) * inv
    top = jnp.max(jnp.abs(out_grad), axis=1, keepdims=True).astype(jnp.bfloat16).astype(jnp.float32)
    top = jnp.where(top > 1e-37, top, 1.0)
    codes = encode(out_grad * (1.0 / top), gain)
    top_wide = jnp.broadcast_to(top, (rows, LANES)).astype(jnp.bfloat16)
    for t in range(dp):
        code[t, :, :feat] = codes[:, t * feat:(t + 1) * feat]
        code[t, :, feat:] = top_wide
        gsend_a[t] = gain_part[:, t * feat:(t + 1) * feat]
    grad[m, d] = code[d]

    pl.semaphore_wait(barrier, dp - 1 + mp - 1)

    def a_copy(j):
        t = lax.rem(d + j, dp)
        return remote(code.at[t], grad.at[m, d], a_send.at[j], a_recv.at[j], (t, m))

    def ga_copy(j):
        t = lax.rem(d + j, dp)
        return remote(gsend_a.at[t], grecv_a.at[j], ga_send.at[j], ga_recv.at[j], (t, m))

    for j in range(1, dp):
        a_copy(j).start()
    for j in range(1, dp):
        ga_copy(j).start()
    for j in range(1, dp):
        a_copy(j).wait_recv()

    def chunk_z(p):
        odd = lax.rem(p, 2)
        off = odd * ((p + 1) // 2) - (1 - odd) * (p // 2)
        return lax.rem(z + off + nz, nz)

    def chunk(k):
        q = lax.rem(k, 2)
        return 2 * chunk_z(k // 2) + lax.rem(y + q, 2)

    def z_copy(p):
        return remote(grad.at[m], grad.at[m], z_send.at[p], g_recv.at[m], (d, 2 * chunk_z(p) + y))

    def y_copy(p):
        mine = 2 * chunk_z(p) + y
        return remote(grad.at[mine], grad.at[mine], y_send.at[p], g_recv.at[mine], (d, 2 * z + 1 - y))

    def g_wait(mc):
        remote(grad.at[mc], grad.at[mc], y_send.at[0], g_recv.at[mc], (d, 2 * z + 1 - y)).wait_recv()

    y_copy(0).start()
    for p in range(1, nz):
        z_copy(p).start()

    for j in range(1, dp):
        ga_copy(j).wait_recv()
    total = gsend_a[d]
    for j in range(1, dp):
        total = total + grecv_a[j]
    gsum[...] = total

    def gb_copy(j):
        return remote(gsum, grecv_b.at[j], gb_send.at[j], gb_recv.at[j], (d, lax.rem(m + j, mp)))

    for j in range(1, mp):
        gb_copy(j).start()

    w_copy.wait()

    def d_copy(k, xo):
        return remote(
            part.at[k, 2 * xo + 1 - core], other.at[k, xo], d_send.at[k, xo], d_recv.at[k, xo], (2 * x + 1 - core, m)
        )

    def x_copy(k, j):
        return remote(
            sent.at[k, j - 1], got.at[k, j - 1], x_send.at[k, j - 1], x_recv.at[k, j - 1],
            (2 * lax.rem(x + j, nx) + core, m),
        )

    def unpack(p):
        for q in range(2):
            mc = chunk(2 * p + q)
            for t in range(dp):
                value = decode(grad[mc, t][:, :feat], gain)
                high = value.astype(jnp.bfloat16)
                at = (2 * t + q) * rows
                lhs[at:at + rows, :] = high
                lhs[2 * dp * rows + at:2 * dp * rows + at + rows, :] = (
                    value - high.astype(jnp.float32)
                ).astype(jnp.bfloat16)

    def compute(k):
        first = lax.rem(k, 2) * half

        def one(i, carry):
            units = pl.ds(pl.multiple_of(first + i * tile, tile), tile)
            cols = pl.ds(pl.multiple_of(i * tile, tile), tile)
            both = lax.dot_general(
                lhs[...], w_ref[units, :], (((1,), (1,)), ((), ())), preferred_element_type=jnp.float32
            )
            both = both[: 2 * dp * rows] + both[2 * dp * rows:]
            for t in range(dp):
                part[k, t, :, cols] = both[2 * t * rows:2 * (t + 1) * rows]
            return carry

        lax.fori_loop(0, half // tile, one, 0)
        for j in range(1, nx + 1):
            d_copy(k, lax.rem(x + j, nx)).start()

    def reduce(k):
        for j in range(1, nx):
            xo = lax.rem(x + j, nx)
            d_copy(k, xo).wait_recv()
            sent[k, j - 1] = encode(part[k, 2 * xo + core] + other[k, xo], gain)
            x_copy(k, j).start()

    def pass_on(p):
        g_wait(chunk(2 * p))
        y_copy(p).start()

    def step(k, carry):
        p, h = k // 2, lax.rem(k, 2)

        @pl.when(h == 0)
        def _():
            g_wait(chunk(k + 1))

            @pl.when(jnp.logical_and(p > 0, p + 1 < nz))
            def _():
                pass_on(p + 1)

            unpack(p)

        compute(k)

        @pl.when(jnp.logical_and(k == 0, nz > 1))
        def _():
            pass_on(1)

        @pl.when(k > 0)
        def _():
            reduce(k - 1)

        return carry

    lax.fori_loop(0, mp, step, 0)
    reduce(mp - 1)

    gtotal = gsum[...]
    for j in range(1, mp):
        gb_copy(j).wait_recv()
        gtotal = gtotal + grecv_b[j]
    gblock[...] = gtotal
    gain_out[d] = gtotal

    def go_copy(j):
        return remote(gblock, gain_out.at[d], go_send.at[j], go_recv.at[j], (lax.rem(d + j, dp), m))

    for j in range(1, dp):
        go_copy(j).start()

    def finish(k, carry):
        p, h = k // 2, lax.rem(k, 2)
        d_copy(k, x).wait_recv()
        for j in range(1, nx):
            x_copy(k, j).wait_recv()
        value = part[k, d] + other[k, x]
        for j in range(1, nx):
            value = value + decode(got[k, j - 1], gain)
        cols = pl.ds(pl.multiple_of(h * half, LANES), half)
        for q in range(2):
            mc = chunk(2 * p + q)
            size = grad[mc, d][:, feat:].astype(jnp.float32)[:, :1]
            out_ref[mc, :, cols] = value[q * rows:(q + 1) * rows] * size
        return carry

    lax.fori_loop(0, mp, finish, 0)

    for j in range(1, dp):
        go_copy(j).wait()
        a_copy(j).wait_send()
        ga_copy(j).wait_send()
    for j in range(1, mp):
        gb_copy(j).wait_send()
    for p in range(nz):
        y_copy(p).wait_send()
    for p in range(1, nz):
        z_copy(p).wait_send()

    def drain(k, carry):
        for xo in range(nx):
            d_copy(k, xo).wait_send()
        for j in range(1, nx):
            x_copy(k, j).wait_send()
        return carry

    lax.fori_loop(0, mp, drain, 0)


def fused(dp, mp, cotangent, mlp_out, post_gain, down_weight):
    rows, full = cotangent.shape
    hid, feat = down_weight.shape
    nx, nz = dp // 2, mp // 2
    gain = 2.0 ** math.floor(15.8 - math.log2(full * WEIGHT_MAX))
    half = hid // 2
    tile = next(t for t in (768, 512, 256, 128) if half % t == 0)
    bf, f32 = jnp.bfloat16, jnp.float32
    dma = pltpu.SemaphoreType.DMA
    hidden, gain_grad = pl.pallas_call(
        functools.partial(kernel, dp, mp, gain, tile),
        out_shape=(jax.ShapeDtypeStruct((mp, rows, hid), f32), jax.ShapeDtypeStruct((dp, 1, feat), f32)),
        in_specs=[pl.BlockSpec(memory_space=pltpu.VMEM)] * 3 + [pl.BlockSpec(memory_space=pl.ANY)],
        out_specs=(pl.BlockSpec(memory_space=pltpu.VMEM), pl.BlockSpec(memory_space=pltpu.VMEM)),
        scratch_shapes=[
            pltpu.VMEM((hid, feat), bf),
            pltpu.VMEM((mp, dp, rows, feat + LANES), bf),
            pltpu.VMEM((dp, rows, feat + LANES), bf),
            pltpu.VMEM((4 * dp * rows, feat), bf),
            pltpu.VMEM((mp, dp, 2 * rows, half), f32),
            pltpu.VMEM((mp, nx, 2 * rows, half), f32),
            pltpu.VMEM((mp, nx - 1, 2 * rows, half), bf),
            pltpu.VMEM((mp, nx - 1, 2 * rows, half), bf),
            pltpu.VMEM((1, feat), f32),
            pltpu.VMEM((dp, 1, feat), f32),
            pltpu.VMEM((dp, 1, feat), f32),
            pltpu.VMEM((mp, 1, feat), f32),
            pltpu.VMEM((1, feat), f32),
            dma, dma((dp,)), dma((dp,)), dma((dp,)), dma((dp,)),
            dma((mp,)), dma((nz,)), dma((nz,)), dma((mp,)), dma((mp,)),
            dma((mp, nx)), dma((mp, nx)), dma((mp, nx)), dma((mp, nx)),
            dma((dp,)), dma((dp,)),
        ],
        compiler_params=pltpu.CompilerParams(
            collective_id=0, has_side_effects=True, vmem_limit_bytes=48 * 1024 * 1024
        ),
        name="norm_gather_project_reduce",
    )(cotangent, mlp_out, post_gain.reshape(1, full), down_weight)
    return hidden.reshape(mp * rows, hid), gain_grad.reshape(full)


def plain(cotangent, mlp_out, post_gain, down_weight):
    full = cotangent.shape[1]
    forward = mlp_out.astype(jnp.float32)
    upstream = cotangent.astype(jnp.float32)
    root_mean = jnp.sqrt(jnp.mean(forward * forward, axis=1, keepdims=True) + epsilon)
    normed = forward / root_mean
    gain_part = jnp.sum(upstream * normed, axis=0)
    scaled = upstream * post_gain[None, :]
    project_sum = jnp.sum(scaled * forward, axis=1, keepdims=True)
    out_grad = scaled / root_mean - forward * project_sum / (full * root_mean**3)
    hid_units = down_weight.shape[0]
    gain_grad = lax.psum(gain_part, ("dp", "mp"))
    pieces = lax.all_to_all(out_grad, "dp", split_axis=1, concat_axis=0, tiled=True)
    partial_value = jnp.dot(
        lax.all_gather(pieces, "mp", axis=0, tiled=True),
        down_weight.astype(jnp.float32).T,
        precision=lax.Precision.HIGHEST,
    )
    dp_count = lax.axis_size("dp")
    mp_count = lax.axis_size("mp")
    row_count = out_grad.shape[0]
    partial_value = partial_value.reshape(mp_count, dp_count * row_count, hid_units)
    summed = lax.psum_scatter(partial_value, "dp", scatter_dimension=1, tiled=True)
    return summed.reshape(mp_count * row_count, hid_units), gain_grad


def local(dp, mp, cotangent, mlp_out, post_gain, down_weight, gate_pre, up_pre):
    rows = cotangent.shape[0]
    hid, feat = down_weight.shape
    held_bytes = mp * rows * hid * (4 * dp + 4 * dp // 2 + 2 * dp + 4) + 2 * hid * feat
    tiled = rows % 16 == 0 and hid % (2 * LANES) == 0 and feat % LANES == 0
    paired = dp % 2 == 0 and mp % 2 == 0 and dp > 2
    if tiled and paired and held_bytes < 40 * 1024 * 1024:
        hidden_grad, gain_grad = fused(dp, mp, cotangent, mlp_out, post_gain, down_weight)
    else:
        hidden_grad, gain_grad = plain(cotangent, mlp_out, post_gain, down_weight)
    gate_val = gate_pre.astype(jnp.float32)
    up_val = up_pre.astype(jnp.float32)
    act_val, pull_back = jax.vjp(gelu_tanh, gate_val)
    gate_grad = pull_back(hidden_grad * up_val)[0]
    up_grad = hidden_grad * act_val
    return (gate_grad, up_grad, gain_grad)


def solution(mesh):
    return jax.shard_map(
        functools.partial(local, mesh.shape["dp"], mesh.shape["mp"]),
        mesh=mesh,
        in_specs=(
            P(("dp", "mp"), None),
            P(("dp", "mp"), None),
            P(),
            P("mp", "dp"),
            P("dp", "mp"),
            P("dp", "mp"),
        ),
        out_specs=(P("dp", "mp"), P("dp", "mp"), P()),
        check_vma=False,
    )
```

```python
import functools
import math

import jax
import jax.numpy as jnp
from jax import lax
from jax.experimental import pallas as pl
from jax.experimental.pallas import tpu as pltpu
from jax.sharding import PartitionSpec as P

MESH = pl.DeviceIdType.MESH
LANES = 128
WEIGHT_MAX = 0.09375

epsilon = 1e-06


def gelu_tanh(values):
    return jax.nn.gelu(values, approximate=True)


def encode(values, gain):
    v = values * gain
    v2 = v * v
    v4 = v2 * v2
    v8 = v4 * v4
    return jnp.where(v < 0, -v8, v8).astype(jnp.bfloat16)


def decode(codes, gain):
    b = codes.astype(jnp.float32)
    size = jnp.abs(b)
    root = jnp.exp(jnp.log(size) * 0.125) * (1.0 / gain)
    root = jnp.where(size > 0, root, 0.0)
    return jnp.where(b < 0, -root, root)


def kernel(
    dp, mp, gain, tile,
    c_hbm, y_hbm, post_ref, w_hbm, out_ref, gain_out,
    c_ref, y_ref, w_ref, grad, code, lhs, part, other, sent, got, gsum, gsend_a, grecv_a, grecv_b, gblock,
    c_sem, y_sem, w_sem, a_send, a_recv, ga_send, ga_recv, g_recv, z_send, y_send, gb_send, gb_recv,
    d_send, d_recv, x_send, x_recv, go_send, go_recv,
):
    d, m = lax.axis_index("dp"), lax.axis_index("mp")
    nx, nz = dp // 2, mp // 2
    x, core = d // 2, lax.rem(d, 2)
    z, y = m // 2, lax.rem(m, 2)
    rows, full = c_ref.shape
    feat = full // dp
    half = w_ref.shape[0] // 2

    def remote(src, dst, send, recv, dev):
        return pltpu.make_async_remote_copy(
            src_ref=src, dst_ref=dst, send_sem=send, recv_sem=recv, device_id=dev, device_id_type=MESH
        )

    c_copy = pltpu.make_async_copy(c_hbm, c_ref, c_sem)
    y_copy_in = pltpu.make_async_copy(y_hbm, y_ref, y_sem)
    w_copy = pltpu.make_async_copy(w_hbm, w_ref, w_sem)
    y_copy_in.start()
    c_copy.start()
    w_copy.start()

    barrier = pltpu.get_barrier_semaphore()
    for j in range(1, dp):
        pl.semaphore_signal(barrier, inc=1, device_id=(lax.rem(d + j, dp), m), device_id_type=MESH)
    for j in range(1, mp):
        pl.semaphore_signal(barrier, inc=1, device_id=(d, lax.rem(m + j, mp)), device_id_type=MESH)

    y_copy_in.wait()
    c_copy.wait()
    forward = y_ref[...].astype(jnp.float32)
    upstream = c_ref[...].astype(jnp.float32)
    inv = 1.0 / jnp.sqrt(jnp.mean(forward * forward, axis=1, keepdims=True) + epsilon)
    normed = forward * inv
    gain_part = jnp.sum(upstream * normed, axis=0, keepdims=True)
    scaled = upstream * post_ref[...]
    mean_prod = jnp.sum(scaled * normed, axis=1, keepdims=True) * (1.0 / full)
    out_grad = (scaled - normed * mean_prod) * inv
    top = jnp.max(jnp.abs(out_grad), axis=1, keepdims=True).astype(jnp.bfloat16).astype(jnp.float32)
    top = jnp.where(top > 1e-37, top, 1.0)
    codes = encode(out_grad * (1.0 / top), gain)
    top_wide = jnp.broadcast_to(top, (rows, LANES)).astype(jnp.bfloat16)
    for t in range(dp):
        code[t, :, :feat] = codes[:, t * feat:(t + 1) * feat]
        code[t, :, feat:] = top_wide
        gsend_a[t] = gain_part[:, t * feat:(t + 1) * feat]
    grad[m, d] = code[d]

    pl.semaphore_wait(barrier, dp - 1 + mp - 1)

    def a_copy(j):
        t = lax.rem(d + j, dp)
        return remote(code.at[t], grad.at[m, d], a_send.at[j], a_recv.at[j], (t, m))

    def ga_copy(j):
        t = lax.rem(d + j, dp)
        return remote(gsend_a.at[t], grecv_a.at[j], ga_send.at[j], ga_recv.at[j], (t, m))

    for j in range(1, dp):
        a_copy(j).start()
    for j in range(1, dp):
        ga_copy(j).start()
    for j in range(1, dp):
        a_copy(j).wait_recv()

    def chunk_z(p):
        odd = lax.rem(p, 2)
        off = odd * ((p + 1) // 2) - (1 - odd) * (p // 2)
        return lax.rem(z + off + nz, nz)

    def chunk(k):
        q = lax.rem(k, 2)
        return 2 * chunk_z(k // 2) + lax.rem(y + q, 2)

    def z_copy(p):
        return remote(grad.at[m], grad.at[m], z_send.at[p], g_recv.at[m], (d, 2 * chunk_z(p) + y))

    def y_copy(p):
        mine = 2 * chunk_z(p) + y
        return remote(grad.at[mine], grad.at[mine], y_send.at[p], g_recv.at[mine], (d, 2 * z + 1 - y))

    def g_wait(mc):
        remote(grad.at[mc], grad.at[mc], y_send.at[0], g_recv.at[mc], (d, 2 * z + 1 - y)).wait_recv()

    y_copy(0).start()
    for p in range(1, nz):
        z_copy(p).start()

    for j in range(1, dp):
        ga_copy(j).wait_recv()
    total = gsend_a[d]
    for j in range(1, dp):
        total = total + grecv_a[j]
    gsum[...] = total

    def gb_copy(j):
        return remote(gsum, grecv_b.at[j], gb_send.at[j], gb_recv.at[j], (d, lax.rem(m + j, mp)))

    for j in range(1, mp):
        gb_copy(j).start()

    w_copy.wait()

    def d_copy(k, xo):
        return remote(
            part.at[k, 2 * xo + 1 - core], other.at[k, xo], d_send.at[k, xo], d_recv.at[k, xo], (2 * x + 1 - core, m)
        )

    def x_copy(k, j):
        return remote(
            sent.at[k, j - 1], got.at[k, j - 1], x_send.at[k, j - 1], x_recv.at[k, j - 1],
            (2 * lax.rem(x + j, nx) + core, m),
        )

    def unpack(p):
        for q in range(2):
            mc = chunk(2 * p + q)
            for t in range(dp):
                value = decode(grad[mc, t][:, :feat], gain)
                high = value.astype(jnp.bfloat16)
                at = (2 * t + q) * rows
                lhs[at:at + rows, :] = high
                lhs[2 * dp * rows + at:2 * dp * rows + at + rows, :] = (
                    value - high.astype(jnp.float32)
                ).astype(jnp.bfloat16)

    def compute(k):
        first = lax.rem(k, 2) * half

        def one(i, carry):
            units = pl.ds(pl.multiple_of(first + i * tile, tile), tile)
            cols = pl.ds(pl.multiple_of(i * tile, tile), tile)
            both = lax.dot_general(
                lhs[...], w_ref[units, :], (((1,), (1,)), ((), ())), preferred_element_type=jnp.float32
            )
            both = both[: 2 * dp * rows] + both[2 * dp * rows:]
            for t in range(dp):
                part[k, t, :, cols] = both[2 * t * rows:2 * (t + 1) * rows]
            return carry

        lax.fori_loop(0, half // tile, one, 0)
        for j in range(1, nx + 1):
            d_copy(k, lax.rem(x + j, nx)).start()

    def reduce(k):
        for j in range(1, nx):
            xo = lax.rem(x + j, nx)
            d_copy(k, xo).wait_recv()
            sent[k, j - 1] = encode(part[k, 2 * xo + core] + other[k, xo], gain)
            x_copy(k, j).start()

    def pass_on(p):
        g_wait(chunk(2 * p))
        y_copy(p).start()

    def step(k, carry):
        p, h = k // 2, lax.rem(k, 2)

        @pl.when(h == 0)
        def _():
            g_wait(chunk(k + 1))

            @pl.when(jnp.logical_and(p > 0, p + 1 < nz))
            def _():
                pass_on(p + 1)

            unpack(p)

        compute(k)

        @pl.when(jnp.logical_and(k == 0, nz > 1))
        def _():
            pass_on(1)

        @pl.when(k == 0)
        def _():
            reduce(k)

        @pl.when(k > 1)
        def _():
            reduce(k - 1)

        return carry

    lax.fori_loop(0, mp, step, 0)
    reduce(mp - 1)

    gtotal = gsum[...]
    for j in range(1, mp):
        gb_copy(j).wait_recv()
        gtotal = gtotal + grecv_b[j]
    gblock[...] = gtotal
    gain_out[d] = gtotal

    def go_copy(j):
        return remote(gblock, gain_out.at[d], go_send.at[j], go_recv.at[j], (lax.rem(d + j, dp), m))

    for j in range(1, dp):
        go_copy(j).start()

    def finish(k, carry):
        p, h = k // 2, lax.rem(k, 2)
        d_copy(k, x).wait_recv()
        for j in range(1, nx):
            x_copy(k, j).wait_recv()
        value = part[k, d] + other[k, x]
        for j in range(1, nx):
            value = value + decode(got[k, j - 1], gain)
        cols = pl.ds(pl.multiple_of(h * half, LANES), half)
        for q in range(2):
            mc = chunk(2 * p + q)
            size = grad[mc, d][:, feat:].astype(jnp.float32)[:, :1]
            out_ref[mc, :, cols] = value[q * rows:(q + 1) * rows] * size
        return carry

    lax.fori_loop(0, mp, finish, 0)

    for j in range(1, dp):
        go_copy(j).wait()
        a_copy(j).wait_send()
        ga_copy(j).wait_send()
    for j in range(1, mp):
        gb_copy(j).wait_send()
    for p in range(nz):
        y_copy(p).wait_send()
    for p in range(1, nz):
        z_copy(p).wait_send()

    def drain(k, carry):
        for xo in range(nx):
            d_copy(k, xo).wait_send()
        for j in range(1, nx):
            x_copy(k, j).wait_send()
        return carry

    lax.fori_loop(0, mp, drain, 0)


def fused(dp, mp, cotangent, mlp_out, post_gain, down_weight):
    rows, full = cotangent.shape
    hid, feat = down_weight.shape
    nx, nz = dp // 2, mp // 2
    gain = 2.0 ** math.floor(15.8 - math.log2(full * WEIGHT_MAX))
    half = hid // 2
    tile = next(t for t in (768, 512, 256, 128) if half % t == 0)
    bf, f32 = jnp.bfloat16, jnp.float32
    dma = pltpu.SemaphoreType.DMA
    hidden, gain_grad = pl.pallas_call(
        functools.partial(kernel, dp, mp, gain, tile),
        out_shape=(jax.ShapeDtypeStruct((mp, rows, hid), f32), jax.ShapeDtypeStruct((dp, 1, feat), f32)),
        in_specs=[pl.BlockSpec(memory_space=s) for s in (pltpu.HBM, pltpu.HBM, pltpu.VMEM, pltpu.HBM)],
        out_specs=(pl.BlockSpec(memory_space=pltpu.VMEM), pl.BlockSpec(memory_space=pltpu.VMEM)),
        scratch_shapes=[
            pltpu.VMEM((rows, full), bf),
            pltpu.VMEM((rows, full), bf),
            pltpu.VMEM((hid, feat), bf),
            pltpu.VMEM((mp, dp, rows, feat + LANES), bf),
            pltpu.VMEM((dp, rows, feat + LANES), bf),
            pltpu.VMEM((4 * dp * rows, feat), bf),
            pltpu.VMEM((mp, dp, 2 * rows, half), f32),
            pltpu.VMEM((mp, nx, 2 * rows, half), f32),
            pltpu.VMEM((mp, nx - 1, 2 * rows, half), bf),
            pltpu.VMEM((mp, nx - 1, 2 * rows, half), bf),
            pltpu.VMEM((1, feat), f32),
            pltpu.VMEM((dp, 1, feat), f32),
            pltpu.VMEM((dp, 1, feat), f32),
            pltpu.VMEM((mp, 1, feat), f32),
            pltpu.VMEM((1, feat), f32),
            dma, dma, dma, dma((dp,)), dma((dp,)), dma((dp,)), dma((dp,)),
            dma((mp,)), dma((nz,)), dma((nz,)), dma((mp,)), dma((mp,)),
            dma((mp, nx)), dma((mp, nx)), dma((mp, nx)), dma((mp, nx)),
            dma((dp,)), dma((dp,)),
        ],
        compiler_params=pltpu.CompilerParams(
            collective_id=0, has_side_effects=True, vmem_limit_bytes=48 * 1024 * 1024
        ),
        name="norm_gather_project_reduce",
    )(cotangent, mlp_out, post_gain.reshape(1, full), down_weight)
    return hidden.reshape(mp * rows, hid), gain_grad.reshape(full)


def plain(cotangent, mlp_out, post_gain, down_weight):
    full = cotangent.shape[1]
    forward = mlp_out.astype(jnp.float32)
    upstream = cotangent.astype(jnp.float32)
    root_mean = jnp.sqrt(jnp.mean(forward * forward, axis=1, keepdims=True) + epsilon)
    normed = forward / root_mean
    gain_part = jnp.sum(upstream * normed, axis=0)
    scaled = upstream * post_gain[None, :]
    project_sum = jnp.sum(scaled * forward, axis=1, keepdims=True)
    out_grad = scaled / root_mean - forward * project_sum / (full * root_mean**3)
    hid_units = down_weight.shape[0]
    gain_grad = lax.psum(gain_part, ("dp", "mp"))
    pieces = lax.all_to_all(out_grad, "dp", split_axis=1, concat_axis=0, tiled=True)
    partial_value = jnp.dot(
        lax.all_gather(pieces, "mp", axis=0, tiled=True),
        down_weight.astype(jnp.float32).T,
        precision=lax.Precision.HIGHEST,
    )
    dp_count = lax.axis_size("dp")
    mp_count = lax.axis_size("mp")
    row_count = out_grad.shape[0]
    partial_value = partial_value.reshape(mp_count, dp_count * row_count, hid_units)
    summed = lax.psum_scatter(partial_value, "dp", scatter_dimension=1, tiled=True)
    return summed.reshape(mp_count * row_count, hid_units), gain_grad


def local(dp, mp, cotangent, mlp_out, post_gain, down_weight, gate_pre, up_pre):
    rows = cotangent.shape[0]
    hid, feat = down_weight.shape
    held_bytes = mp * rows * hid * (4 * dp + 4 * dp // 2 + 2 * dp + 4) + 2 * hid * feat
    tiled = rows % 16 == 0 and hid % (2 * LANES) == 0 and feat % LANES == 0
    paired = dp % 2 == 0 and mp % 2 == 0 and dp > 2
    if tiled and paired and held_bytes < 40 * 1024 * 1024:
        hidden_grad, gain_grad = fused(dp, mp, cotangent, mlp_out, post_gain, down_weight)
    else:
        hidden_grad, gain_grad = plain(cotangent, mlp_out, post_gain, down_weight)
    gate_val = gate_pre.astype(jnp.float32)
    up_val = up_pre.astype(jnp.float32)
    act_val, pull_back = jax.vjp(gelu_tanh, gate_val)
    gate_grad = pull_back(hidden_grad * up_val)[0]
    up_grad = hidden_grad * act_val
    return (gate_grad, up_grad, gain_grad)


def solution(mesh):
    return jax.shard_map(
        functools.partial(local, mesh.shape["dp"], mesh.shape["mp"]),
        mesh=mesh,
        in_specs=(
            P(("dp", "mp"), None),
            P(("dp", "mp"), None),
            P(),
            P("mp", "dp"),
            P("dp", "mp"),
            P("dp", "mp"),
        ),
        out_specs=(P("dp", "mp"), P("dp", "mp"), P()),
        check_vma=False,
    )
```
